32 devices in a mesh: dp: 8 (over y, x, core), tensor: 4 (over z).
Axes of the slice: x: 2, y: 2, z: 4, core: 2. Of those that a mesh axis runs over, the one named last changes fastest.
Arguments:
- inputs: bfloat16 [8192, 2048], P(('dp', 'tensor')), may hold values from -22 to 22
- segments: int32 [8, 1024], P('dp'), may hold values from 0 to 7, never falling along the last dimension, each value on 1 to 512 neighbouring positions
- first_gain: float32 [2048], replicated, may hold values from 0.5 to 1.5
- first_shift: float32 [2048], replicated, may hold values from -4 to 4
- second_gain: float32 [2048], replicated, may hold values from 0.5 to 1.5
- second_shift: float32 [2048], replicated, may hold values from -4 to 4
- qkv_weight: bfloat16 [2048, 8, 3, 256], P('dp', 'tensor'), may hold values from -3 to 3
- qkv_bias: float32 [8, 3, 256], P('tensor'), may hold values from -3 to 3
- dense_weight: bfloat16 [2048, 2048], P('dp', 'tensor'), may hold values from -0.5 to 0.5
- dense_bias: float32 [2048], replicated, may hold values from -4 to 4
- fc_weight: bfloat16 [2048, 8192], P('dp', 'tensor'), may hold values from -0.125 to 0.125
- fc_bias: float32 [8192], P('tensor'), may hold values from -3 to 3
- proj_weight: bfloat16 [2048, 8192], P('dp', 'tensor'), may hold values from -0.0625 to 0.0625
- proj_bias: float32 [2048], replicated, may hold values from -4 to 4
- cotangent: bfloat16 [8192, 2048], P(('dp', 'tensor')), may hold values from -6 to 6
Outputs:
- output: bfloat16 [8192, 2048], P(('dp', 'tensor'))
- input_grad: bfloat16 [8192, 2048], P(('dp', 'tensor'))
- first_gain_grad: float32 [2048], replicated
- first_shift_grad: float32 [2048], replicated
- second_gain_grad: float32 [2048], replicated
- second_shift_grad: float32 [2048], replicated
- qkv_weight_grad: float32 [2048, 8, 3, 256], P('dp', 'tensor')
- qkv_bias_grad: float32 [8, 3, 256], P('tensor')
- dense_weight_grad: float32 [2048, 2048], P('dp', 'tensor')
- dense_bias_grad: float32 [2048], replicated
- fc_weight_grad: float32 [2048, 8192], P('dp', 'tensor')
- fc_bias_grad: float32 [8192], P('tensor')
- proj_weight_grad: float32 [2048, 8192], P('dp', 'tensor')
- proj_bias_grad: float32 [2048], replicated
The draws below stay inside these ranges and needn't reach their ends.
Inputs may be any that keep to these rules, and one draw needn't show every extreme that they name: `segments`: within a sequence segment numbers never fall.
All inputs are finite; a program needn't handle non-finite values.
Results may differ from the reference program's by a relative error of at most 0.015.
The reference program's roundings to bfloat16 on the way count: a program that leaves them out, or rounds other values in their place, can miss the bound.
Values may be sent and summed in bfloat16 or wider, within the bound.
A program may use at most 192 MiB of HBM per device.

```python
import math
import jax
import jax.numpy as jnp
import numpy as np
from jax import lax

D = 2048
H = 8
HD = 256
ROT = 64
FF = 8192
SEQ = 1024
SEGS = 8
SEQS = 8
TOKENS = 8192


def draw_inputs(key, part):
    base = jnp.clip(jax.random.normal(jax.random.fold_in(key, 1), (TOKENS, D), jnp.float32), -4.0, 4.0)
    return base.astype(jnp.bfloat16)


def draw_qkv_weight(key, part):
    base = jnp.clip(jax.random.normal(jax.random.fold_in(key, 5), (D, H, 3, HD), jnp.float32), -5.0, 5.0) * D ** (-0.5)
    return base.astype(jnp.bfloat16)


def level_of(own_key, dims, split, low, top_value):
    loudness = 1.0
    for dim, blocks in split:
        heights = jax.random.uniform(jax.random.fold_in(jax.random.fold_in(own_key, 6), dim), (blocks,), jnp.float32, low / len(split), top_value / len(split))
        loudness = loudness * jnp.repeat(jnp.exp(heights), dims[dim] // blocks).reshape((-1,) + (1,) * (len(dims) - 1 - dim))
    return loudness


def length_profile(count, total, most, lean):
    portions = [(1 << 20) // math.isqrt(rank ** lean) + 1 for rank in range(2, count + 1)]
    surplus, counts = total - most - (count - 1), [1] * (count - 1)
    while surplus > 0:
        candidates = [i for i in range(count - 1) if counts[i] < most]
        whole, remaining = sum([portions[i] for i in candidates]), surplus
        for i in candidates:
            extra = min(most - counts[i], max(1, remaining * portions[i] // whole), surplus)
            counts[i] = counts[i] + extra
            surplus = surplus - extra
    return np.array([most] + counts)


def ragged_sizes(own_key, count, total, limit, lean):
    if count == 2:
        one = jax.random.randint(own_key, (), max(1, total - limit), min(limit, total - 1) + 1)
        return jnp.stack([one, total - one])
    sizes = jnp.asarray(length_profile(count, total, limit, lean), jnp.int32)
    pairs = (count - 1) // 2
    source_of, taker = sizes[1:1 + 2 * pairs:2], sizes[2:2 + 2 * pairs:2]
    room = jnp.minimum(source_of - 1, limit - taker)
    shifted = jax.random.randint(jax.random.fold_in(own_key, 1), (pairs,), 0, 1 << 20) % (room + 1)
    sizes = sizes.at[1:1 + 2 * pairs:2].set(source_of - shifted).at[2:2 + 2 * pairs:2].set(taker + shifted)
    return sizes[jax.random.permutation(jax.random.fold_in(own_key, 2), count)]


def bell_draw(rng, dims, deviation, most, split=(), kind=jnp.bfloat16):
    result = deviation * jax.random.normal(rng, dims, jnp.float32)
    if split:
        result = result * level_of(rng, dims, split, -0.22, 0.18)
    return jnp.clip(result, -most, most).astype(kind)


def setup_inputs(seed: int = 0) -> dict:
    arg_keys = jax.random.split(jax.random.key(seed), 16)
    return {
        "inputs": draw_inputs(jax.random.fold_in(arg_keys[15], 71), 0),
        "segments": jax.vmap(lambda own: jnp.searchsorted(jnp.cumsum(ragged_sizes(own, SEGS, SEQ, SEQ // 2, 2)), jnp.arange(SEQ), side="right"))(jax.random.split(arg_keys[1], SEQS)).reshape((SEQS, SEQ)).astype(jnp.int32),
        "first_gain": jnp.clip(1.0 + 0.1 * jax.random.normal(arg_keys[2], (D,), jnp.float32), 0.5, 1.5),
        "first_shift": bell_draw(arg_keys[3], (D,), 0.3, 4.0, (), jnp.float32),
        "second_gain": jnp.clip(1.0 + 0.1 * jax.random.normal(arg_keys[4], (D,), jnp.float32), 0.5, 1.5),
        "second_shift": bell_draw(arg_keys[5], (D,), 0.3, 4.0, (), jnp.float32),
        "qkv_weight": draw_qkv_weight(jax.random.fold_in(arg_keys[15], 71), 0),
        "qkv_bias": bell_draw(arg_keys[7], (H, 3, HD), 0.5, 3.0, ((0, 4),), jnp.float32),
        "dense_weight": bell_draw(arg_keys[8], (D, H * HD), (H * HD // 16) ** -0.5, 0.5, ((0, 8), (1, 4))),
        "dense_bias": bell_draw(arg_keys[9], (D,), 0.3, 4.0, (), jnp.float32),
        "fc_weight": bell_draw(arg_keys[10], (D, FF), D ** -0.5, 0.125, ((0, 8), (1, 4))),
        "fc_bias": bell_draw(arg_keys[11], (FF,), 0.5, 3.0, ((0, 4),), jnp.float32),
        "proj_weight": bell_draw(arg_keys[12], (D, FF), FF ** -0.5, 0.0625, ((0, 8), (1, 4))),
        "proj_bias": bell_draw(arg_keys[13], (D,), 0.3, 4.0, (), jnp.float32),
        "cotangent": bell_draw(arg_keys[14], (TOKENS, D), 1.0, 6.0, ((0, 32),)),
    }


norm_eps = 1e-05
erf_scale = 0.7071067811865476
normal_peak = 0.3989422804014327

def normalize(layer_input):
    widened = layer_input.astype(jnp.float32)
    centred = widened - lax.optimization_barrier(jnp.mean(widened, axis=-1, keepdims=True))
    inv_scale = lax.rsqrt(lax.optimization_barrier(jnp.mean(centred * centred, axis=-1, keepdims=True)) + norm_eps)
    return (centred * inv_scale, inv_scale)

def norm_back(d_normed, unit_rows, inv_scale, gain):
    scaled = d_normed * gain
    first_mean = lax.optimization_barrier(jnp.mean(scaled, axis=-1, keepdims=True))
    second_mean = lax.optimization_barrier(jnp.mean(scaled * unit_rows, axis=-1, keepdims=True))
    return inv_scale * (scaled - first_mean - unit_rows * second_mean)

def gelu_value(pre_act):
    return 0.5 * pre_act * (1.0 + lax.erf(pre_act * erf_scale))

def gelu_slope(pre_act):
    return 0.5 * (1.0 + lax.erf(pre_act * erf_scale)) + pre_act * jnp.exp(-0.5 * pre_act * pre_act) * normal_peak

def rotary_tables(segment):
    length = segment.shape[0]
    places = jnp.arange(length, dtype=jnp.int32)
    changed = jnp.concatenate([jnp.ones((1,), dtype=bool), segment[1:] != segment[:-1]])
    starts = lax.cummax(jnp.where(changed, places, 0), axis=0)
    position = (places - starts).astype(jnp.float32)
    frequency = 10000.0 ** (-jnp.arange(0, ROT, 2).astype(jnp.float32) / ROT)
    angles = position[:, None] * frequency[None, :]
    angles = jnp.concatenate([angles, angles], axis=-1)
    return (jnp.cos(angles), jnp.sin(angles))

def rotate(vectors, cosine, sine_part):
    half_rot = ROT // 2
    rot_front = vectors[..., :ROT]
    turned = jnp.concatenate([-rot_front[..., half_rot:], rot_front[..., :half_rot]], axis=-1)
    return jnp.concatenate([rot_front * cosine + turned * sine_part, vectors[..., ROT:]], axis=-1)

def rotate_back(grad_rows, cosine, sine_part):
    half_rot = ROT // 2
    rot_front = grad_rows[..., :ROT]
    lifted = rot_front * sine_part
    turned = jnp.concatenate([lifted[..., half_rot:], -lifted[..., :half_rot]], axis=-1)
    return jnp.concatenate([rot_front * cosine + turned, grad_rows[..., ROT:]], axis=-1)

def contract_first(left_side, right_side):
    return lax.dot_general(left_side, right_side, (((0,), (0,)), ((), ())), preferred_element_type=jnp.float32)

def contract_last(left_side, right_side):
    return lax.dot_general(left_side, right_side, (((1,), (1,)), ((), ())), preferred_element_type=jnp.float32)

def masked_scores(query_rows, key_rows, segment, first_row):
    block_len = query_rows.shape[0]
    scores = contract_last(query_rows, key_rows) * HD ** (-0.5)
    row_ids = first_row + jnp.arange(block_len)
    col_ids = jnp.arange(key_rows.shape[0])
    own_segment = segment[first_row:first_row + block_len]
    allowed = (col_ids[None, :] <= row_ids[:, None]) & (segment[None, :] == own_segment[:, None])
    return jnp.where(allowed, scores, -jnp.inf)

def attend(queries, keyed, valued, segment):
    length = queries.shape[0]
    block_len = min(512, length)
    context_parts = []
    total_parts = []
    for first_row in range(0, length, block_len):
        row_end = first_row + block_len
        scores = masked_scores(queries[first_row:row_end], keyed[:row_end], segment[:row_end], first_row)
        row_peak = lax.optimization_barrier(jnp.max(scores, axis=-1, keepdims=True))
        exp_terms = jnp.exp(scores - row_peak)
        row_total = lax.optimization_barrier(jnp.sum(exp_terms, axis=-1, keepdims=True))
        weights = (exp_terms / row_total).astype(jnp.bfloat16)
        context_parts.append(jnp.dot(weights, valued[:row_end], preferred_element_type=jnp.float32).astype(jnp.bfloat16))
        total_parts.append(row_peak[:, 0] + jnp.log(row_total[:, 0]))
    return (jnp.concatenate(context_parts, axis=0), jnp.concatenate(total_parts, axis=0))

def attend_back(queries, keyed, valued, segment, context, log_total, d_context):
    length = queries.shape[0]
    block_len = min(512, length)
    delta_rows = lax.optimization_barrier(jnp.sum(d_context.astype(jnp.float32) * context.astype(jnp.float32), axis=-1))
    d_keys = jnp.zeros(keyed.shape, jnp.float32)
    d_values = jnp.zeros(valued.shape, jnp.float32)
    query_parts = []
    for first_row in range(0, length, block_len):
        row_end = first_row + block_len
        scores = masked_scores(queries[first_row:row_end], keyed[:row_end], segment[:row_end], first_row)
        prob_rows = jnp.exp(scores - log_total[first_row:row_end, None])
        d_rows = d_context[first_row:row_end]
        value_term = contract_first(prob_rows.astype(jnp.bfloat16), d_rows)
        d_values = d_values + jnp.pad(value_term, ((0, length - row_end), (0, 0)))
        d_probs = contract_last(d_rows, valued[:row_end])
        d_scores = (prob_rows * (d_probs - delta_rows[first_row:row_end, None]) * HD ** (-0.5)).astype(jnp.bfloat16)
        query_parts.append(jnp.dot(d_scores, keyed[:row_end], preferred_element_type=jnp.float32))
        key_term = contract_first(d_scores, queries[first_row:row_end])
        d_keys = d_keys + jnp.pad(key_term, ((0, length - row_end), (0, 0)))
    return (jnp.concatenate(query_parts, axis=0), d_keys, d_values)

def split_heads(qkv_rows, cosine, sine_part, head_count, seq_count):
    qkv_parts = qkv_rows.reshape(seq_count, SEQ, head_count, 3, HD).transpose(3, 2, 0, 1, 4)
    queries = rotate(qkv_parts[0], cosine, sine_part).astype(jnp.bfloat16)
    keyed = rotate(qkv_parts[1], cosine, sine_part).astype(jnp.bfloat16)
    valued = qkv_parts[2].astype(jnp.bfloat16)
    return (queries, keyed, valued)

def merge_heads(per_head):
    head_count, seq_count = (per_head.shape[0], per_head.shape[1])
    return per_head.transpose(1, 2, 0, 3).reshape(seq_count * SEQ, head_count * HD)

def join_grads(d_queries, d_keys, d_values):
    head_count, seq_count = (d_queries.shape[0], d_queries.shape[1])
    stacked = jnp.stack([d_queries, d_keys, d_values], axis=0)
    return stacked.transpose(2, 3, 1, 0, 4).reshape(seq_count * SEQ, head_count * 3 * HD)

def reference(inputs, segments, first_gain, first_shift, second_gain, second_shift, qkv_weight, qkv_bias, dense_weight, dense_bias, fc_weight, fc_bias, proj_weight, proj_bias, cotangent):
    model_width = inputs.shape[1]
    head_count = qkv_weight.shape[1]
    qkv_flat = qkv_weight.reshape(model_width, head_count * 3 * HD)
    attend_all = jax.vmap(jax.vmap(attend), in_axes=(0, 0, 0, None))
    attend_back_all = jax.vmap(jax.vmap(attend_back), in_axes=(0, 0, 0, None, 0, 0, 0))

    def advance(totals, sequence):
        seq_inputs, seq_cot, segment = sequence
        segment_rows = segment[None]
        cosine, sine_part = jax.vmap(rotary_tables)(segment_rows)
        unit_rows, inv_scale = normalize(seq_inputs)
        first_normed = (unit_rows * first_gain + first_shift).astype(jnp.bfloat16)
        second_normed = (unit_rows * second_gain + second_shift).astype(jnp.bfloat16)
        qkv_rows = jnp.dot(first_normed, qkv_flat, preferred_element_type=jnp.float32) + qkv_bias.reshape(-1)
        queries, keyed, valued = split_heads(qkv_rows, cosine, sine_part, head_count, 1)
        context, log_total = attend_all(queries, keyed, valued, segment_rows)
        context_rows = merge_heads(context)
        pre_act = jnp.dot(second_normed, fc_weight, preferred_element_type=jnp.float32) + fc_bias
        activated = gelu_value(pre_act).astype(jnp.bfloat16)
        attn_part = contract_last(context_rows, dense_weight)
        mlp_part = contract_last(activated, proj_weight)
        output = (seq_inputs.astype(jnp.float32) + attn_part + mlp_part + dense_bias + proj_bias).astype(jnp.bfloat16)
        cot_wide = seq_cot.astype(jnp.float32)
        bias_grad = lax.optimization_barrier(jnp.sum(cot_wide, axis=0))
        proj_grad = contract_first(seq_cot, activated)
        d_act = jnp.dot(seq_cot, proj_weight, preferred_element_type=jnp.float32)
        d_pre = d_act * gelu_slope(pre_act)
        fc_bias_part = lax.optimization_barrier(jnp.sum(d_pre, axis=0))
        d_pre_half = d_pre.astype(jnp.bfloat16)
        fc_grad = contract_first(second_normed, d_pre_half)
        d_second = contract_last(d_pre_half, fc_weight)
        dense_grad = contract_first(seq_cot, context_rows)
        d_context = jnp.dot(seq_cot, dense_weight, preferred_element_type=jnp.float32).astype(jnp.bfloat16)
        d_context_heads = d_context.reshape(1, SEQ, head_count, HD).transpose(2, 0, 1, 3)
        d_queries, d_keys, d_values = attend_back_all(queries, keyed, valued, segment_rows, context, log_total, d_context_heads)
        d_queries = rotate_back(d_queries, cosine, sine_part)
        d_keys = rotate_back(d_keys, cosine, sine_part)
        d_qkv = join_grads(d_queries, d_keys, d_values)
        qkv_bias_part = lax.optimization_barrier(jnp.sum(d_qkv, axis=0)).reshape(head_count, 3, HD)
        d_qkv_half = d_qkv.astype(jnp.bfloat16)
        qkv_grad = contract_first(first_normed, d_qkv_half).reshape(model_width, head_count, 3, HD)
        d_first = contract_last(d_qkv_half, qkv_flat)
        first_gain_part = lax.optimization_barrier(jnp.sum(d_first * unit_rows, axis=0))
        first_shift_part = lax.optimization_barrier(jnp.sum(d_first, axis=0))
        second_gain_part = lax.optimization_barrier(jnp.sum(d_second * unit_rows, axis=0))
        second_shift_part = lax.optimization_barrier(jnp.sum(d_second, axis=0))
        input_grad = (cot_wide + norm_back(d_first, unit_rows, inv_scale, first_gain) + norm_back(d_second, unit_rows, inv_scale, second_gain)).astype(jnp.bfloat16)
        new_parts = (first_gain_part, first_shift_part, second_gain_part, second_shift_part, qkv_grad, qkv_bias_part, dense_grad, bias_grad, fc_grad, fc_bias_part, proj_grad)
        return (tuple((left_part + right_part for left_part, right_part in zip(totals, new_parts))), (output, input_grad))
    zero_totals = (jnp.zeros((model_width,), jnp.float32), jnp.zeros((model_width,), jnp.float32), jnp.zeros((model_width,), jnp.float32), jnp.zeros((model_width,), jnp.float32), jnp.zeros(qkv_weight.shape, jnp.float32), jnp.zeros(qkv_bias.shape, jnp.float32), jnp.zeros(dense_weight.shape, jnp.float32), jnp.zeros((model_width,), jnp.float32), jnp.zeros(fc_weight.shape, jnp.float32), jnp.zeros(fc_bias.shape, jnp.float32), jnp.zeros(proj_weight.shape, jnp.float32))
    seq_inputs_all = inputs.reshape(SEQS, SEQ, model_width)
    seq_cot_all = cotangent.reshape(SEQS, SEQ, model_width)
    totals, (outputs, input_grads) = lax.scan(advance, zero_totals, (seq_inputs_all, seq_cot_all, segments))
    return (outputs.reshape(TOKENS, model_width), input_grads.reshape(TOKENS, model_width), totals[0], totals[1], totals[2], totals[3], totals[4], totals[5], totals[6], totals[7], totals[8], totals[9], totals[10], totals[7])
```

```python
import functools

import jax
import jax.numpy as jnp
from jax import lax
from jax.experimental import pallas as pl
from jax.experimental.pallas import tpu as pltpu
from jax.sharding import PartitionSpec as P

MESH = pl.DeviceIdType.MESH
ROT = 64
CORES = 2


norm_eps = 1e-05
erf_scale = 0.7071067811865476
normal_peak = 0.3989422804014327


def snake_at(place, n):
    upper = lax.div(place, n // 2)
    return place + upper * (3 * n // 2 - 1 - 2 * place)


def snake_place(index, n):
    return snake_at(index, n)


def comb_at(place, n):
    upper = lax.div(place, n // 2)
    return (1 - upper) * 2 * place + upper * (2 * (n - 1 - place) + 1)


def comb_place(index, n):
    odd = lax.rem(index, 2)
    half = lax.div(index, 2)
    return (1 - odd) * half + odd * (n - 1 - half)


def static_order(kind, n):
    if kind == "snake":
        return list(range(n // 2)) + list(range(n - 1, n // 2 - 1, -1))
    return list(range(0, n, 2)) + list(range(n - 1, 0, -2))


class Gather:
    def __init__(self, src, dst, rows, n, index_of, to_right, to_left, partner, sems):
        self.src, self.dst, self.rows, self.n = src, dst, rows, n
        self.index_of, self.right, self.left, self.partner = index_of, to_right, to_left, partner
        self.local_sem, self.send_sems, self.recv_sems = sems
        self.used = 0
        self.hops = {}
        self.mates = []
        self.sent = []

    def part(self, index, half):
        size = self.rows // 2
        return self.dst.at[pl.ds(pl.multiple_of(index * self.rows + half * size, size), size), :]

    def push(self, src, dst, device):
        copy = pltpu.make_async_remote_copy(
            src_ref=src,
            dst_ref=dst,
            send_sem=self.send_sems.at[self.used],
            recv_sem=self.recv_sems.at[self.used],
            device_id=device,
            device_id_type=MESH,
        )
        self.used += 1
        copy.start()
        self.sent.append(copy)
        return copy

    def own(self):
        size = self.rows // 2
        index = self.index_of(0)
        self.local = pltpu.make_async_copy(
            self.src, self.dst.at[pl.ds(pl.multiple_of(index * self.rows, self.rows), self.rows), :], self.local_sem
        )
        self.local.start()
        for first in (0, 1):
            for side, device in ((0, self.right), (1, self.left)):
                half = first if side == 0 else 1 - first
                if self.n == 2 and side != half:
                    continue
                if self.n == 2:
                    pass
                source = self.src.at[pl.ds(half * size, size), :]
                self.hops[(1, side, half)] = self.push(source, self.part(index, half), device)
        if self.partner is not None:
            for half in (0, 1):
                source = self.src.at[pl.ds(half * size, size), :]
                self.mates.append(self.push(source, self.part(index, half), self.partner))

    def step(self, step):
        for first in (0, 1):
            for side in (0, 1):
                half = first if side == 0 else 1 - first
                key = (step, side, half)
                if key not in self.hops:
                    continue
                self.hops[key].wait_recv()
                index = self.index_of(-step if side == 0 else step)
                block = self.part(index, half)
                last = step + 1 == self.n // 2
                if step < self.n // 2 and (not last or first == 0):
                    self.hops[(step + 1, side, half)] = self.push(block, block, self.right if side == 0 else self.left)
                if self.partner is not None:
                    self.mates.append(self.push(block, block, self.partner))

    def end(self):
        for copy in self.mates:
            copy.wait_recv()
        self.local.wait()
        for copy in self.sent:
            copy.wait_send()


def copies_of(n, mates):
    hops = 4 * (n // 2 - 1) + 2 if n > 2 else 2
    return hops + (2 * n if mates else 0)


def gather_kernel(nz, nr, x_ref, qkv_ref, fc_ref, dense_ref, proj_ref, cot_ref, *refs):
    outs, sems = refs[:6], refs[6:]
    dp, z = lax.axis_index("dp"), lax.axis_index("tensor")
    chip, core = lax.div(dp, CORES), lax.rem(dp, CORES)
    zp, rp = snake_place(z, nz), comb_place(chip, nr)

    def z_at(k):
        return snake_at(lax.rem(zp + k + nz, nz), nz)

    def r_at(k):
        return comb_at(lax.rem(rp + k + nr, nr), nr) * CORES + core

    z_right, z_left = (dp, z_at(1)), (dp, z_at(-1))
    r_right, r_left = (r_at(1), z), (r_at(-1), z)
    mate = (chip * CORES + 1 - core, z)

    barrier = pltpu.get_barrier_semaphore()
    neighbours = [z_right, z_left, r_right, r_left, mate]
    for device in neighbours:
        pl.semaphore_signal(barrier, inc=1, device_id=device, device_id_type=MESH)
    pl.semaphore_wait(barrier, len(neighbours))

    def along_z(src, k):
        return Gather(src, outs[k], src.shape[0], nz, z_at, z_right, z_left, None, sems[3 * k : 3 * k + 3])

    def along_r(src, k):
        return Gather(src, outs[k], src.shape[0], nr, r_at, r_right, r_left, mate, sems[3 * k : 3 * k + 3])

    tokens, cot = along_z(x_ref, 0), along_z(cot_ref, 5)
    weights = [along_r(ref, k + 1) for k, ref in enumerate((qkv_ref, fc_ref, dense_ref, proj_ref))]
    tokens.own()
    weights[0].own()
    weights[1].own()
    for step in range(1, nz // 2):
        tokens.step(step)
    cot.own()
    for step in range(1, nr // 2 + 1):
        weights[0].step(step)
    tokens.step(nz // 2)
    weights[2].own()
    weights[3].own()
    for step in range(1, nr // 2 + 1):
        weights[1].step(step)
    for step in range(1, nz // 2 + 1):
        cot.step(step)
    for weight in weights[2:]:
        for step in range(1, nr // 2 + 1):
            weight.step(step)
    for task in [tokens, cot] + weights:
        task.end()


def gather_all(x, qkv, fc, dense, proj, cot):
    nz, nr = lax.axis_size("tensor"), lax.axis_size("dp") // CORES
    arrays = (x, qkv, fc, dense, proj, cot)
    times = (nz,) + (nr * CORES,) * 4 + (nz,)
    scratch = []
    for k in range(6):
        count = copies_of(nz, False) if k in (0, 5) else copies_of(nr, True)
        scratch += [pltpu.SemaphoreType.DMA, pltpu.SemaphoreType.DMA((count,)), pltpu.SemaphoreType.DMA((count,))]
    return pl.pallas_call(
        functools.partial(gather_kernel, nz, nr),
        out_shape=[jax.ShapeDtypeStruct((a.shape[0] * t, a.shape[1]), a.dtype) for a, t in zip(arrays, times)],
        in_specs=[pl.BlockSpec(memory_space=pltpu.VMEM)] * 6,
        out_specs=[pl.BlockSpec(memory_space=pl.ANY)] * 6,
        scratch_shapes=scratch,
        compiler_params=pltpu.CompilerParams(collective_id=0, has_side_effects=True),
        name="gather_all",
    )(*arrays)


def turned(front):
    lane = lax.broadcasted_iota(jnp.int32, front.shape, 1)
    width = front.shape[1]
    return jnp.where(lane < ROT // 2, pltpu.roll(front, width - ROT // 2, 1), pltpu.roll(front, ROT // 2, 1))


def rotary_tables(segment, width):
    length = segment.shape[0]
    starts = jnp.sum((segment[None, :] < segment[:, None]).astype(jnp.int32), axis=1)
    position = (jnp.arange(length, dtype=jnp.int32) - starts).astype(jnp.float32)
    frequency = 10000.0 ** (-jnp.arange(0, ROT, 2).astype(jnp.float32) / ROT)
    angles = position[:, None] * frequency[None, :]
    cosine, sine = jnp.cos(angles), jnp.sin(angles)
    rest = width - ROT
    cos_table = jnp.concatenate([cosine, cosine, jnp.ones((length, rest), jnp.float32)], axis=1)
    sin_table = jnp.concatenate([-sine, sine, jnp.zeros((length, rest), jnp.float32)], axis=1)
    return cos_table, sin_table


def key_range(block, rows, reach):
    return max(0, (block * rows - reach + 1) // rows * rows), (block + 1) * rows


def allowed_of(col_seg, row_seg, first, low, high, rows):
    row_ids = first + lax.broadcasted_iota(jnp.int32, (rows, high - low), 0)
    col_ids = low + lax.broadcasted_iota(jnp.int32, (rows, high - low), 1)
    return (col_ids <= row_ids) & (row_seg[:, low:high] == col_seg[first : first + rows, :])


def contract_last(left, right):
    return lax.dot_general(left, right, (((1,), (1,)), ((), ())), preferred_element_type=jnp.float32)


def contract_first(left, right):
    return lax.dot_general(left, right, (((0,), (0,)), ((), ())), preferred_element_type=jnp.float32)


def attend_kernel(hd, rows, reach, qkv_ref, cos_ref, sin_ref, row_seg, col_seg, q_ref, k_ref, v_ref, ctx_ref, log_ref):
    length = qkv_ref.shape[0]
    wide = cos_ref.shape[1]
    cosine, sine = cos_ref[...], sin_ref[...]
    for part, out in ((0, q_ref), (1, k_ref)):
        front = qkv_ref[:, part * hd : part * hd + wide]
        out[:, :wide] = (front * cosine + turned(front) * sine).astype(jnp.bfloat16)
        out[:, wide:] = qkv_ref[:, part * hd + wide : (part + 1) * hd].astype(jnp.bfloat16)
    v_ref[...] = qkv_ref[:, 2 * hd :].astype(jnp.bfloat16)
    for block in range(length // rows):
        first = block * rows
        low, high = key_range(block, rows, reach)
        scores = contract_last(q_ref[first : first + rows, :], k_ref[low:high, :]) * hd ** (-0.5)
        allowed = allowed_of(col_seg, row_seg, first, low, high, rows)
        scores = jnp.where(allowed, scores, -jnp.inf)
        peak = jnp.max(scores, axis=-1, keepdims=True)
        terms = jnp.exp(scores - peak)
        total = jnp.sum(terms, axis=-1, keepdims=True)
        weights = (terms / total).astype(jnp.bfloat16)
        ctx_ref[first : first + rows, :] = jnp.dot(
            weights, v_ref[low:high, :], preferred_element_type=jnp.float32
        ).astype(jnp.bfloat16)
        log_ref[0, first : first + rows, :] = peak + jnp.log(total)


def attend_back_kernel(
    hd, rows, reach, q_ref, k_ref, v_ref, ctx_ref, log_ref, dctx_ref, cos_ref, sin_ref, row_seg, col_seg,
    out_ref, bias_ref, dk_acc, dv_acc,
):
    length = q_ref.shape[0]
    wide = cos_ref.shape[1]
    dk_acc[...] = jnp.zeros_like(dk_acc)
    dv_acc[...] = jnp.zeros_like(dv_acc)

    def put(part, first, grad, count):
        front = grad[:, :wide]
        front = front * cos_ref[first : first + count, :] - turned(front) * sin_ref[first : first + count, :]
        out_ref[first : first + count, part * hd : part * hd + wide] = front.astype(jnp.bfloat16)
        out_ref[first : first + count, part * hd + wide : (part + 1) * hd] = grad[:, wide:].astype(jnp.bfloat16)
        sums = jnp.concatenate(
            [jnp.sum(front, axis=0, keepdims=True), jnp.sum(grad[:, wide:], axis=0, keepdims=True)], axis=1
        )
        if first == 0:
            bias_ref[:, part * hd : (part + 1) * hd] = sums
        else:
            bias_ref[:, part * hd : (part + 1) * hd] += sums

    for block in range(length // rows):
        first = block * rows
        low, high = key_range(block, rows, reach)
        own = slice(first, first + rows)
        queries, d_rows = q_ref[own, :], dctx_ref[own, :]
        delta = jnp.sum(d_rows.astype(jnp.float32) * ctx_ref[own, :].astype(jnp.float32), axis=-1, keepdims=True)
        scores = contract_last(queries, k_ref[low:high, :]) * hd ** (-0.5)
        allowed = allowed_of(col_seg, row_seg, first, low, high, rows)
        probs = jnp.where(allowed, jnp.exp(scores - log_ref[0, own, :]), 0.0)
        dv_acc[low:high, :] += contract_first(probs.astype(jnp.bfloat16), d_rows)
        d_probs = contract_last(d_rows, v_ref[low:high, :])
        d_scores = (probs * (d_probs - delta) * hd ** (-0.5)).astype(jnp.bfloat16)
        put(0, first, jnp.dot(d_scores, k_ref[low:high, :], preferred_element_type=jnp.float32), rows)
        dk_acc[low:high, :] += contract_first(d_scores, queries)
    for block in range(length // rows):
        first = block * rows
        put(1, first, dk_acc[first : first + rows, :], rows)
        grad = dv_acc[first : first + rows, :]
        out_ref[first : first + rows, 2 * hd :] = grad.astype(jnp.bfloat16)
        sums = jnp.sum(grad, axis=0, keepdims=True)
        if first == 0:
            bias_ref[:, 2 * hd :] = sums
        else:
            bias_ref[:, 2 * hd :] += sums


def attend(qkv_rows, tables, segment, heads, hd, rows, reach):
    length = qkv_rows.shape[0]
    row_seg, col_seg = segment[None, :], segment[:, None]
    whole = lambda a: pl.BlockSpec(a.shape, lambda h: (0,) * a.ndim)
    column = pl.BlockSpec((length, hd), lambda h: (0, h))
    per_head = jax.ShapeDtypeStruct((length, heads * hd), jnp.bfloat16)
    return pl.pallas_call(
        functools.partial(attend_kernel, hd, rows, reach),
        grid=(heads,),
        in_specs=[pl.BlockSpec((length, 3 * hd), lambda h: (0, h))]
        + [whole(a) for a in (*tables, row_seg, col_seg)],
        out_specs=[column] * 4 + [pl.BlockSpec((1, length, 1), lambda h: (h, 0, 0))],
        out_shape=[per_head] * 4 + [jax.ShapeDtypeStruct((heads, length, 1), jnp.float32)],
        name="attend",
    )(qkv_rows, *tables, row_seg, col_seg)


def attend_back(saved, log_total, d_context, tables, segment, heads, hd, rows, reach):
    length = d_context.shape[0]
    row_seg, col_seg = segment[None, :], segment[:, None]
    whole = lambda a: pl.BlockSpec(a.shape, lambda h: (0,) * a.ndim)
    column = pl.BlockSpec((length, hd), lambda h: (0, h))
    return pl.pallas_call(
        functools.partial(attend_back_kernel, hd, rows, reach),
        grid=(heads,),
        in_specs=[column] * 4
        + [pl.BlockSpec((1, length, 1), lambda h: (h, 0, 0)), column]
        + [whole(a) for a in (*tables, row_seg, col_seg)],
        out_specs=[pl.BlockSpec((length, 3 * hd), lambda h: (0, h)), pl.BlockSpec((1, 3 * hd), lambda h: (0, h))],
        out_shape=[
            jax.ShapeDtypeStruct((length, heads * 3 * hd), jnp.bfloat16),
            jax.ShapeDtypeStruct((1, heads * 3 * hd), jnp.float32),
        ],
        scratch_shapes=[pltpu.VMEM((length, hd), jnp.float32)] * 2,
        name="attend_back",
    )(*saved, log_total, d_context, *tables, row_seg, col_seg)


def ring_scatter(block_of, shift, n):
    to_bf16 = lambda a: a.astype(jnp.bfloat16)
    wide = lambda a: a.astype(jnp.float32)
    far = block_of(n // 2)
    half = far.shape[0] // 2
    right, left = shift(to_bf16(far[:half]), 1), shift(to_bf16(far[half:]), -1)
    for k in range(n // 2 - 1, 0, -1):
        ahead, behind = block_of(k), block_of(-k)
        if right.shape[0] == half:
            ahead = jnp.concatenate([ahead[:half] + wide(right), ahead[half:]])
            behind = jnp.concatenate([behind[:half], behind[half:] + wide(left)])
        else:
            ahead, behind = ahead + wide(right), behind + wide(left)
        right, left = shift(to_bf16(ahead), 1), shift(to_bf16(behind), -1)
    return block_of(0) + wide(right) + wide(left)


def summed(vector, axis):
    n = lax.axis_size(axis)
    bit = 1
    while bit < n:
        vector = vector + lax.ppermute(vector, axis, [(i, i ^ bit) for i in range(n)])
        bit *= 2
    return vector


def gelu_value(pre_act):
    return 0.5 * pre_act * (1.0 + lax.erf(pre_act * erf_scale))


def gelu_slope(pre_act):
    return (
        0.5 * (1.0 + lax.erf(pre_act * erf_scale))
        + pre_act * jnp.exp(-0.5 * pre_act * pre_act) * normal_peak
    )


def per_device(
    inputs,
    segments,
    first_gain,
    first_shift,
    second_gain,
    second_shift,
    qkv_weight,
    qkv_bias,
    dense_weight,
    dense_bias,
    fc_weight,
    fc_bias,
    proj_weight,
    proj_bias,
    cotangent,
):
    shard, heads, _, hd = qkv_weight.shape
    width = inputs.shape[1]
    rows = inputs.shape[0]
    nz, nd = lax.axis_size("tensor"), lax.axis_size("dp")
    nr = nd // CORES
    length = segments.shape[1]
    z, dp = lax.axis_index("tensor"), lax.axis_index("dp")
    chip, core = dp // CORES, dp % CORES
    f32, bf16 = jnp.float32, jnp.bfloat16

    all_in, qkv_w, fc_w, dense_w, proj_w, all_cot = gather_all(
        inputs, qkv_weight.reshape(shard, heads * 3 * hd), fc_weight, dense_weight, proj_weight, cotangent
    )
    segment = segments[0]
    tables = rotary_tables(segment, 128)

    wide_in = all_in.astype(f32)
    mean = jnp.mean(wide_in, axis=-1, keepdims=True)
    centred = wide_in - mean
    inv_scale = lax.rsqrt(jnp.mean(centred * centred, axis=-1, keepdims=True) + norm_eps)
    unit = centred * inv_scale
    first_normed = (unit * first_gain + first_shift).astype(bf16)
    second_normed = (unit * second_gain + second_shift).astype(bf16)

    qkv_rows = jnp.dot(first_normed, qkv_w, preferred_element_type=f32) + qkv_bias.reshape(-1)
    block_rows = min(256, length)
    *saved, log_total = attend(qkv_rows, tables, segment, heads, hd, block_rows, length // 2)
    context = saved[3]
    pre_act = jnp.dot(second_normed, fc_w, preferred_element_type=f32) + fc_bias
    activated = gelu_value(pre_act).astype(bf16)

    z_order = static_order("snake", nz)
    z_place = snake_place(z, nz)
    z_index = lambda k: snake_at((z_place + k + nz) % nz, nz)

    def z_shift(a, d):
        return lax.ppermute(a, "tensor", [(z_order[i], z_order[(i + d) % nz]) for i in range(nz)])

    r_order = static_order("comb", nr)
    r_place = comb_place(chip, nr)
    r_index = lambda k: comb_at((r_place + k + nr) % nr, nr)

    def r_shift(a, d):
        pairs = [
            (r_order[i] * CORES + c, r_order[(i + d) % nr] * CORES + c) for i in range(nr) for c in range(CORES)
        ]
        return lax.ppermute(a, "dp", pairs)

    def rows_of(a):
        return lambda k: lax.dynamic_slice_in_dim(a, z_index(k) * rows, rows, axis=0).astype(f32)

    mixed_part = (contract_last(context, dense_w) + contract_last(activated, proj_w)).astype(bf16)
    mixed = ring_scatter(rows_of(mixed_part), z_shift, nz)
    output = (inputs.astype(f32) + mixed + dense_bias + proj_bias).astype(bf16)

    def weight_scatter(grad):
        grad = grad.reshape(nr, CORES, shard, -1)
        mates = lax.dynamic_index_in_dim(grad, 1 - core, 1, keepdims=False)
        mine = lax.dynamic_index_in_dim(grad, core, 1, keepdims=False)
        got = lax.ppermute(mates, "dp", [(i, i ^ 1) for i in range(nd)])

        def block_of(k):
            take = lambda a: lax.dynamic_index_in_dim(a, r_index(k), 0, keepdims=False).astype(f32)
            return take(mine) + take(got)

        return ring_scatter(block_of, r_shift, nr)

    proj_grad = contract_first(all_cot, activated).astype(bf16)
    proj_weight_grad = weight_scatter(proj_grad)
    d_act = jnp.dot(all_cot, proj_w, preferred_element_type=f32)
    d_pre = d_act * gelu_slope(pre_act)
    fc_bias_part = jnp.sum(d_pre, axis=0)
    d_pre_half = d_pre.astype(bf16)
    fc_grad = contract_first(second_normed, d_pre_half).astype(bf16)
    fc_weight_grad = weight_scatter(fc_grad)
    d_context = jnp.dot(all_cot, dense_w, preferred_element_type=f32).astype(bf16)
    dense_grad = contract_first(all_cot, context).astype(bf16)
    dense_weight_grad = weight_scatter(dense_grad)
    d_qkv_half, qkv_bias_part = attend_back(
        saved, log_total, d_context, tables, segment, heads, hd, block_rows, length // 2
    )
    d_second = contract_last(d_pre_half, fc_w)
    d_first = contract_last(d_qkv_half, qkv_w)
    joint = (d_first * first_gain + d_second * second_gain).astype(bf16)
    joint_rows = ring_scatter(rows_of(joint), z_shift, nz)
    qkv_grad = contract_first(first_normed, d_qkv_half).astype(bf16)
    qkv_weight_grad = weight_scatter(qkv_grad)

    own = lambda a: lax.dynamic_slice_in_dim(a, z * rows, rows, axis=0)
    own_unit = (inputs.astype(f32) - own(mean)) * own(inv_scale)
    first_mean = jnp.mean(joint_rows, axis=-1, keepdims=True)
    second_mean = jnp.mean(joint_rows * own_unit, axis=-1, keepdims=True)
    input_grad = (
        cotangent.astype(f32) + own(inv_scale) * (joint_rows - first_mean - own_unit * second_mean)
    ).astype(bf16)

    gains = jnp.stack(
        [
            jnp.sum(d_first * unit, axis=0),
            jnp.sum(d_first, axis=0),
            jnp.sum(d_second * unit, axis=0),
            jnp.sum(d_second, axis=0),
        ]
    )
    gains = summed(summed(gains, "dp"), "tensor")
    early = jnp.concatenate([jnp.sum(all_cot.astype(f32), axis=0), fc_bias_part, qkv_bias_part[0]])
    early = summed(early, "dp")
    bias_total = early[:width]
    fc_bias_grad = early[width : width + fc_bias.shape[0]]
    qkv_bias_grad = early[width + fc_bias.shape[0] :].reshape(qkv_bias.shape)
    return (
        output,
        input_grad,
        gains[0],
        gains[1],
        gains[2],
        gains[3],
        qkv_weight_grad.reshape(qkv_weight.shape),
        qkv_bias_grad,
        dense_weight_grad,
        bias_total,
        fc_weight_grad,
        fc_bias_grad,
        proj_weight_grad,
        bias_total,
    )


def solution(mesh):
    both = P(("dp", "tensor"), None)
    return jax.shard_map(
        per_device,
        mesh=mesh,
        in_specs=(
            both,
            P("dp", None),
            P(),
            P(),
            P(),
            P(),
            P("dp", "tensor", None, None),
            P("tensor", None, None),
            P("dp", "tensor"),
            P(),
            P("dp", "tensor"),
            P("tensor"),
            P("dp", "tensor"),
            P(),
            both,
        ),
        out_specs=(
            both,
            both,
            P(),
            P(),
            P(),
            P(),
            P("dp", "tensor", None, None),
            P("tensor", None, None),
            P("dp", "tensor"),
            P(),
            P("dp", "tensor"),
            P("tensor"),
            P("dp", "tensor"),
            P(),
        ),
        check_vma=False,
    )
```

```python
import functools
import math

import jax
import jax.numpy as jnp
from jax import lax
from jax.experimental import pallas as pl
from jax.experimental.pallas import tpu as pltpu
from jax.sharding import PartitionSpec as P

MESH = pl.DeviceIdType.MESH
ROT = 64
CORES = 2


norm_eps = 1e-05
erf_scale = 0.7071067811865476
normal_peak = 0.3989422804014327


def snake_at(place, n):
    upper = lax.div(place, n // 2)
    return place + upper * (3 * n // 2 - 1 - 2 * place)


def snake_place(index, n):
    return snake_at(index, n)


def comb_at(place, n):
    upper = lax.div(place, n // 2)
    return (1 - upper) * 2 * place + upper * (2 * (n - 1 - place) + 1)


def comb_place(index, n):
    odd = lax.rem(index, 2)
    half = lax.div(index, 2)
    return (1 - odd) * half + odd * (n - 1 - half)


def static_order(kind, n):
    if kind == "snake":
        return list(range(n // 2)) + list(range(n - 1, n // 2 - 1, -1))
    return list(range(0, n, 2)) + list(range(n - 1, 0, -2))


class Gather:
    def __init__(self, src, dst, first, n, index_of, to_right, to_left, partner, sems):
        self.src, self.dst, self.n = src, dst, n
        self.rows, self.columns = src.shape[0], pl.ds(first, src.shape[1])
        self.index_of, self.right, self.left, self.partner = index_of, to_right, to_left, partner
        self.local_sem, self.send_sems, self.recv_sems = sems
        self.used = 0
        self.hops = {}
        self.mates = []
        self.sent = []

    def part(self, index, half):
        size = self.rows // 2
        return self.dst.at[pl.ds(pl.multiple_of(index * self.rows + half * size, size), size), self.columns]

    def push(self, src, dst, device):
        copy = pltpu.make_async_remote_copy(
            src_ref=src,
            dst_ref=dst,
            send_sem=self.send_sems.at[self.used],
            recv_sem=self.recv_sems.at[self.used],
            device_id=device,
            device_id_type=MESH,
        )
        self.used += 1
        copy.start()
        self.sent.append(copy)
        return copy

    def own(self):
        size = self.rows // 2
        index = self.index_of(0)
        self.local = pltpu.make_async_copy(
            self.src,
            self.dst.at[pl.ds(pl.multiple_of(index * self.rows, self.rows), self.rows), self.columns],
            self.local_sem,
        )
        self.local.start()
        for first in (0, 1):
            for side, device in ((0, self.right), (1, self.left)):
                half = first if side == 0 else 1 - first
                if self.n == 2 and side != half:
                    continue
                source = self.src.at[pl.ds(half * size, size), :]
                self.hops[(1, side, half)] = self.push(source, self.part(index, half), device)
        if self.partner is not None:
            for half in (0, 1):
                source = self.src.at[pl.ds(half * size, size), :]
                self.mates.append(self.push(source, self.part(index, half), self.partner))

    def step(self, step):
        for first in (0, 1):
            for side in (0, 1):
                half = first if side == 0 else 1 - first
                key = (step, side, half)
                if key not in self.hops:
                    continue
                self.hops[key].wait_recv()
                index = self.index_of(-step if side == 0 else step)
                block = self.part(index, half)
                last = step + 1 == self.n // 2
                if step < self.n // 2 and (not last or first == 0):
                    self.hops[(step + 1, side, half)] = self.push(block, block, self.right if side == 0 else self.left)
                if self.partner is not None:
                    self.mates.append(self.push(block, block, self.partner))

    def end(self):
        for copy in self.mates:
            copy.wait_recv()
        self.local.wait()
        for copy in self.sent:
            copy.wait_send()


def copies_of(n, mates):
    hops = 4 * (n // 2 - 1) + 2 if n > 2 else 2
    return hops + (2 * n if mates else 0)


def gather_kernel(nr, *refs):
    srcs, outs, sems = refs[:4], refs[4:6], refs[6:]
    dp, z = lax.axis_index("dp"), lax.axis_index("tensor")
    chip, core = lax.div(dp, CORES), lax.rem(dp, CORES)
    place = comb_place(chip, nr)

    def at(k):
        return comb_at(lax.rem(place + k + nr, nr), nr) * CORES + core

    right, left = (at(1), z), (at(-1), z)
    mate = (chip * CORES + 1 - core, z)

    barrier = pltpu.get_barrier_semaphore()
    neighbours = [right, left, mate]
    for device in neighbours:
        pl.semaphore_signal(barrier, inc=1, device_id=device, device_id_type=MESH)
    pl.semaphore_wait(barrier, len(neighbours))

    weights = [
        Gather(
            src, outs[k // 2], (k % 2) * srcs[k - 1].shape[1], nr, at, right, left, mate, sems[3 * k : 3 * k + 3]
        )
        for k, src in enumerate(srcs)
    ]
    weights[0].own()
    weights[1].own()
    for step in range(1, nr // 2 + 1):
        weights[0].step(step)
    weights[2].own()
    weights[3].own()
    for weight in weights[1:]:
        for step in range(1, nr // 2 + 1):
            weight.step(step)
    for task in weights:
        task.end()


def gather_weights(arrays):
    nr = lax.axis_size("dp") // CORES
    rows, kind = arrays[0].shape[0] * nr * CORES, arrays[0].dtype
    count = copies_of(nr, True)
    return pl.pallas_call(
        functools.partial(gather_kernel, nr),
        out_shape=[
            jax.ShapeDtypeStruct((rows, arrays[k].shape[1] + arrays[k + 1].shape[1]), kind) for k in (0, 2)
        ],
        in_specs=[pl.BlockSpec(memory_space=pltpu.VMEM)] * 4,
        out_specs=[pl.BlockSpec(memory_space=pl.ANY)] * 2,
        scratch_shapes=[
            pltpu.SemaphoreType.DMA,
            pltpu.SemaphoreType.DMA((count,)),
            pltpu.SemaphoreType.DMA((count,)),
        ]
        * 4,
        compiler_params=pltpu.CompilerParams(collective_id=0, has_side_effects=True),
        name="gather_weights",
    )(*arrays)


def turned(front):
    lane = lax.broadcasted_iota(jnp.int32, front.shape, 1)
    width = front.shape[1]
    return jnp.where(lane < ROT // 2, pltpu.roll(front, width - ROT // 2, 1), pltpu.roll(front, ROT // 2, 1))


def rotary_tables(segment, width):
    length = segment.shape[0]
    starts = jnp.sum((segment[None, :] < segment[:, None]).astype(jnp.int32), axis=1)
    position = (jnp.arange(length, dtype=jnp.int32) - starts).astype(jnp.float32)
    frequency = 10000.0 ** (-jnp.arange(0, ROT, 2).astype(jnp.float32) / ROT)
    angles = position[:, None] * frequency[None, :]
    cosine, sine = jnp.cos(angles), jnp.sin(angles)
    rest = width - ROT
    cos_table = jnp.concatenate([cosine, cosine, jnp.ones((length, rest), jnp.float32)], axis=1)
    sin_table = jnp.concatenate([-sine, sine, jnp.zeros((length, rest), jnp.float32)], axis=1)
    return cos_table, sin_table


def key_range(block, rows, reach):
    return max(0, (block * rows - reach + 1) // rows * rows), (block + 1) * rows


def allowed_of(col_seg, row_seg, first, low, high, rows):
    row_ids = first + lax.broadcasted_iota(jnp.int32, (rows, high - low), 0)
    col_ids = low + lax.broadcasted_iota(jnp.int32, (rows, high - low), 1)
    return (col_ids <= row_ids) & (row_seg[:, low:high] == col_seg[first : first + rows, :])


def contract_last(left, right):
    return lax.dot_general(left, right, (((1,), (1,)), ((), ())), preferred_element_type=jnp.float32)


def contract_first(left, right):
    return lax.dot_general(left, right, (((0,), (0,)), ((), ())), preferred_element_type=jnp.float32)


def attend_kernel(hd, rows, reach, qkv_ref, cos_ref, sin_ref, row_seg, col_seg, q_ref, k_ref, v_ref, ctx_ref, log_ref):
    length = qkv_ref.shape[0]
    wide = cos_ref.shape[1]
    cosine, sine = cos_ref[...], sin_ref[...]
    for part, out in ((0, q_ref), (1, k_ref)):
        front = qkv_ref[:, part * hd : part * hd + wide]
        out[:, :wide] = (front * cosine + turned(front) * sine).astype(jnp.bfloat16)
        out[:, wide:] = qkv_ref[:, part * hd + wide : (part + 1) * hd].astype(jnp.bfloat16)
    v_ref[...] = qkv_ref[:, 2 * hd :].astype(jnp.bfloat16)
    for block in range(length // rows):
        first = block * rows
        low, high = key_range(block, rows, reach)
        scores = contract_last(q_ref[first : first + rows, :], k_ref[low:high, :]) * hd ** (-0.5)
        allowed = allowed_of(col_seg, row_seg, first, low, high, rows)
        scores = jnp.where(allowed, scores, -jnp.inf)
        peak = jnp.max(scores, axis=-1, keepdims=True)
        terms = jnp.exp(scores - peak)
        total = jnp.sum(terms, axis=-1, keepdims=True)
        weights = (terms / total).astype(jnp.bfloat16)
        ctx_ref[first : first + rows, :] = jnp.dot(
            weights, v_ref[low:high, :], preferred_element_type=jnp.float32
        ).astype(jnp.bfloat16)
        log_ref[0, first : first + rows, :] = peak + jnp.log(total)


def attend_back_kernel(
    hd, rows, reach, q_ref, k_ref, v_ref, ctx_ref, log_ref, dctx_ref, cos_ref, sin_ref, row_seg, col_seg,
    out_ref, bias_ref, dk_acc, dv_acc,
):
    length = q_ref.shape[0]
    wide = cos_ref.shape[1]
    dk_acc[...] = jnp.zeros_like(dk_acc)
    dv_acc[...] = jnp.zeros_like(dv_acc)

    def put(part, first, grad, count):
        front = grad[:, :wide]
        front = front * cos_ref[first : first + count, :] - turned(front) * sin_ref[first : first + count, :]
        out_ref[first : first + count, part * hd : part * hd + wide] = front.astype(jnp.bfloat16)
        out_ref[first : first + count, part * hd + wide : (part + 1) * hd] = grad[:, wide:].astype(jnp.bfloat16)
        sums = jnp.concatenate(
            [jnp.sum(front, axis=0, keepdims=True), jnp.sum(grad[:, wide:], axis=0, keepdims=True)], axis=1
        )
        if first == 0:
            bias_ref[:, part * hd : (part + 1) * hd] = sums
        else:
            bias_ref[:, part * hd : (part + 1) * hd] += sums

    for block in range(length // rows):
        first = block * rows
        low, high = key_range(block, rows, reach)
        own = slice(first, first + rows)
        queries, d_rows = q_ref[own, :], dctx_ref[own, :]
        delta = jnp.sum(d_rows.astype(jnp.float32) * ctx_ref[own, :].astype(jnp.float32), axis=-1, keepdims=True)
        scores = contract_last(queries, k_ref[low:high, :]) * hd ** (-0.5)
        allowed = allowed_of(col_seg, row_seg, first, low, high, rows)
        probs = jnp.where(allowed, jnp.exp(scores - log_ref[0, own, :]), 0.0)
        dv_acc[low:high, :] += contract_first(probs.astype(jnp.bfloat16), d_rows)
        d_probs = contract_last(d_rows, v_ref[low:high, :])
        d_scores = (probs * (d_probs - delta) * hd ** (-0.5)).astype(jnp.bfloat16)
        put(0, first, jnp.dot(d_scores, k_ref[low:high, :], preferred_element_type=jnp.float32), rows)
        dk_acc[low:high, :] += contract_first(d_scores, queries)
    for block in range(length // rows):
        first = block * rows
        put(1, first, dk_acc[first : first + rows, :], rows)
        grad = dv_acc[first : first + rows, :]
        out_ref[first : first + rows, 2 * hd :] = grad.astype(jnp.bfloat16)
        sums = jnp.sum(grad, axis=0, keepdims=True)
        if first == 0:
            bias_ref[:, 2 * hd :] = sums
        else:
            bias_ref[:, 2 * hd :] += sums


def attend(qkv_rows, tables, segment, heads, hd, rows, reach):
    length = qkv_rows.shape[0]
    row_seg, col_seg = segment[None, :], segment[:, None]
    whole = lambda a: pl.BlockSpec(a.shape, lambda h: (0,) * a.ndim)
    column = pl.BlockSpec((length, hd), lambda h: (0, h))
    per_head = jax.ShapeDtypeStruct((length, heads * hd), jnp.bfloat16)
    return pl.pallas_call(
        functools.partial(attend_kernel, hd, rows, reach),
        grid=(heads,),
        in_specs=[pl.BlockSpec((length, 3 * hd), lambda h: (0, h))]
        + [whole(a) for a in (*tables, row_seg, col_seg)],
        out_specs=[column] * 4 + [pl.BlockSpec((1, length, 1), lambda h: (h, 0, 0))],
        out_shape=[per_head] * 4 + [jax.ShapeDtypeStruct((heads, length, 1), jnp.float32)],
        name="attend",
    )(qkv_rows, *tables, row_seg, col_seg)


def attend_back(saved, log_total, d_context, tables, segment, heads, hd, rows, reach):
    length = d_context.shape[0]
    row_seg, col_seg = segment[None, :], segment[:, None]
    whole = lambda a: pl.BlockSpec(a.shape, lambda h: (0,) * a.ndim)
    column = pl.BlockSpec((length, hd), lambda h: (0, h))
    return pl.pallas_call(
        functools.partial(attend_back_kernel, hd, rows, reach),
        grid=(heads,),
        in_specs=[column] * 4
        + [pl.BlockSpec((1, length, 1), lambda h: (h, 0, 0)), column]
        + [whole(a) for a in (*tables, row_seg, col_seg)],
        out_specs=[pl.BlockSpec((length, 3 * hd), lambda h: (0, h)), pl.BlockSpec((1, 3 * hd), lambda h: (0, h))],
        out_shape=[
            jax.ShapeDtypeStruct((length, heads * 3 * hd), jnp.bfloat16),
            jax.ShapeDtypeStruct((1, heads * 3 * hd), jnp.float32),
        ],
        scratch_shapes=[pltpu.VMEM((length, hd), jnp.float32)] * 2,
        name="attend_back",
    )(*saved, log_total, d_context, *tables, row_seg, col_seg)


def row_loop(count, step, body):
    def at(i, _):
        body(pl.multiple_of(i * step, step))

    lax.fori_loop(0, count // step, at, None)


def front_kernel(
    qkv_tiles, norm_rows, mat_rows, x_ref, w_ref, bias_ref, gain1, shift1, gain2, shift2,
    qkv_ref, act_ref, slope_ref, n1_ref, n2_ref, mean_ref, inv_ref, got, ssem, rsem,
):
    step = pl.program_id(0)
    length = x_ref.shape[0]
    dp, z = lax.axis_index("dp"), lax.axis_index("tensor")
    mate = (dp + 1 - 2 * lax.rem(dp, CORES), z)
    copy = pltpu.make_async_remote_copy(src_ref=gain1, dst_ref=got, send_sem=ssem, recv_sem=rsem, device_id=mate, device_id_type=MESH)

    @pl.when(step == 0)
    def _():
        barrier = pltpu.get_barrier_semaphore()
        pl.semaphore_signal(barrier, inc=1, device_id=mate, device_id_type=MESH)
        pl.semaphore_wait(barrier, 1)
        copy.start()

    @pl.when(step == pl.num_programs(0) - 1)
    def _():
        copy.wait()

    @pl.when(step == 0)
    def _():
        def normalise(first):
            own = pl.ds(first, norm_rows)
            wide = x_ref[own, :].astype(jnp.float32)
            mean = jnp.mean(wide, axis=-1, keepdims=True)
            centred = wide - mean
            inv = lax.rsqrt(jnp.mean(centred * centred, axis=-1, keepdims=True) + norm_eps)
            unit = centred * inv
            n1_ref[own, :] = (unit * gain1[...] + shift1[...]).astype(jnp.bfloat16)
            n2_ref[own, :] = (unit * gain2[...] + shift2[...]).astype(jnp.bfloat16)
            mean_ref[own, :] = mean
            inv_ref[own, :] = inv

        row_loop(length, norm_rows, normalise)

    @pl.when(step < qkv_tiles)
    def _():
        def rows(first):
            own = pl.ds(first, mat_rows)
            qkv_ref[own, :] = (
                jnp.dot(n1_ref[own, :], w_ref[...], preferred_element_type=jnp.float32) + bias_ref[...]
            )

        row_loop(length, mat_rows, rows)

    @pl.when(step >= qkv_tiles)
    def _():
        def rows(first):
            own = pl.ds(first, mat_rows)
            pre = jnp.dot(n2_ref[own, :], w_ref[...], preferred_element_type=jnp.float32) + bias_ref[...]
            half_erf = 0.5 * (1.0 + lax.erf(pre * erf_scale))
            act_ref[own, :] = (pre * half_erf).astype(jnp.bfloat16)
            slope_ref[own, :] = half_erf + pre * jnp.exp(-0.5 * pre * pre) * normal_peak

        row_loop(length, mat_rows, rows)


def front(x, w, bias, vectors, qkv_cols):
    length, width = x.shape
    cols = w.shape[1]
    hidden = cols - qkv_cols
    tile = math.gcd(qkv_cols, hidden)
    n_qkv = qkv_cols // tile
    once = lambda shape: pl.BlockSpec(shape, lambda i: (0, 0))
    wide_row = once((1, width))
    first = lambda i: (0, jnp.minimum(i, n_qkv - 1))
    second = lambda i: (0, jnp.maximum(i - n_qkv, 0))
    f32, bf16 = jnp.float32, jnp.bfloat16
    return pl.pallas_call(
        functools.partial(front_kernel, n_qkv, min(64, length), min(512, length)),
        grid=(cols // tile,),
        in_specs=[
            once((length, width)),
            pl.BlockSpec((width, tile), lambda i: (0, i)),
            pl.BlockSpec((1, tile), lambda i: (0, i)),
        ]
        + [wide_row] * 4,
        out_specs=[
            pl.BlockSpec((length, tile), first),
            pl.BlockSpec((length, tile), second),
            pl.BlockSpec((length, tile), second),
            once((length, width)),
            once((length, width)),
            once((length, 1)),
            once((length, 1)),
        ],
        out_shape=[
            jax.ShapeDtypeStruct((length, qkv_cols), f32),
            jax.ShapeDtypeStruct((length, hidden), bf16),
            jax.ShapeDtypeStruct((length, hidden), f32),
            jax.ShapeDtypeStruct((length, width), bf16),
            jax.ShapeDtypeStruct((length, width), bf16),
            jax.ShapeDtypeStruct((length, 1), f32),
            jax.ShapeDtypeStruct((length, 1), f32),
        ],
        cost_estimate=pl.CostEstimate(
            flops=2 * length * width * cols,
            bytes_accessed=2 * width * cols + 6 * length * width + 4 * length * cols,
            transcendentals=2 * length * hidden,
        ),
        scratch_shapes=[pltpu.VMEM((1, width), f32), pltpu.SemaphoreType.DMA, pltpu.SemaphoreType.DMA],
        compiler_params=pltpu.CompilerParams(collective_id=1, has_side_effects=True),
        name="front",
    )(x, w, bias, *vectors)


def mix_kernel(mat_rows, ctx_ref, act_ref, w_ref, out_ref):
    split = ctx_ref.shape[1]

    def rows(first):
        own = pl.ds(first, mat_rows)
        out_ref[own, :] = (
            contract_last(ctx_ref[own, :], w_ref[:, :split]) + contract_last(act_ref[own, :], w_ref[:, split:])
        ).astype(jnp.bfloat16)

    row_loop(ctx_ref.shape[0], mat_rows, rows)


def mix(ctx, act, w):
    length = ctx.shape[0]
    width, cols = w.shape
    tile = min(256, width)
    return pl.pallas_call(
        functools.partial(mix_kernel, min(512, length)),
        grid=(width // tile,),
        in_specs=[
            pl.BlockSpec(ctx.shape, lambda i: (0, 0)),
            pl.BlockSpec(act.shape, lambda i: (0, 0)),
            pl.BlockSpec((tile, cols), lambda i: (i, 0)),
        ],
        out_specs=pl.BlockSpec((length, tile), lambda i: (0, i)),
        out_shape=jax.ShapeDtypeStruct((length, width), jnp.bfloat16),
        cost_estimate=pl.CostEstimate(
            flops=2 * length * width * cols,
            bytes_accessed=2 * (width * cols + length * cols + length * width),
            transcendentals=0,
        ),
        name="mix",
    )(ctx, act, w)


def back_kernel(n_ctx, mat_rows, cot_ref, w_ref, slope_ref, dctx_ref, dpre_ref, bias_ref):
    step = pl.program_id(0)
    length = cot_ref.shape[0]

    @pl.when(step < n_ctx)
    def _():
        def rows(first):
            own = pl.ds(first, mat_rows)
            dctx_ref[own, :] = jnp.dot(cot_ref[own, :], w_ref[...], preferred_element_type=jnp.float32).astype(
                jnp.bfloat16
            )

        row_loop(length, mat_rows, rows)

    @pl.when(step >= n_ctx)
    def _():
        bias_ref[...] = jnp.zeros_like(bias_ref)

        def rows(first):
            own = pl.ds(first, mat_rows)
            grad = jnp.dot(cot_ref[own, :], w_ref[...], preferred_element_type=jnp.float32) * slope_ref[own, :]
            dpre_ref[own, :] = grad.astype(jnp.bfloat16)
            bias_ref[...] += jnp.sum(grad, axis=0, keepdims=True)

        row_loop(length, mat_rows, rows)


def back(cot, w, slope, ctx_cols):
    length, width = cot.shape
    cols = w.shape[1]
    hidden = cols - ctx_cols
    tile = math.gcd(ctx_cols, hidden)
    n_ctx = ctx_cols // tile
    first = lambda i: (0, jnp.minimum(i, n_ctx - 1))
    second = lambda i: (0, jnp.maximum(i - n_ctx, 0))
    return pl.pallas_call(
        functools.partial(back_kernel, n_ctx, min(512, length)),
        grid=(cols // tile,),
        in_specs=[
            pl.BlockSpec((length, width), lambda i: (0, 0)),
            pl.BlockSpec((width, tile), lambda i: (0, i)),
            pl.BlockSpec((length, tile), second),
        ],
        out_specs=[
            pl.BlockSpec((length, tile), first),
            pl.BlockSpec((length, tile), second),
            pl.BlockSpec((1, tile), second),
        ],
        out_shape=[
            jax.ShapeDtypeStruct((length, ctx_cols), jnp.bfloat16),
            jax.ShapeDtypeStruct((length, hidden), jnp.bfloat16),
            jax.ShapeDtypeStruct((1, hidden), jnp.float32),
        ],
        cost_estimate=pl.CostEstimate(
            flops=2 * length * width * cols,
            bytes_accessed=2 * (width * cols + length * cols + length * width) + 4 * length * hidden,
            transcendentals=0,
        ),
        name="back",
    )(cot, w, slope)


def joint_kernel(mat_rows, dqkv_ref, dpre_ref, w_ref, x_ref, mean_ref, inv_ref, gain1, gain2, out_ref, sums_ref):
    split = dqkv_ref.shape[1]
    sums_ref[...] = jnp.zeros_like(sums_ref)

    def rows(first):
        own = pl.ds(first, mat_rows)
        d_first = contract_last(dqkv_ref[own, :], w_ref[:, :split])
        d_second = contract_last(dpre_ref[own, :], w_ref[:, split:])
        unit = (x_ref[own, :].astype(jnp.float32) - mean_ref[own, :]) * inv_ref[own, :]
        out_ref[own, :] = (d_first * gain1[...] + d_second * gain2[...]).astype(jnp.bfloat16)
        for k, term in enumerate((d_first * unit, d_first, d_second * unit, d_second)):
            sums_ref[k : k + 1, :] += jnp.sum(term, axis=0, keepdims=True)

    row_loop(dqkv_ref.shape[0], mat_rows, rows)


def joint_sum(dqkv, dpre, w, x, mean, inv, gain1, gain2):
    length = x.shape[0]
    width, cols = w.shape
    tile = min(256, width)
    whole = lambda a: pl.BlockSpec(a.shape, lambda i: (0, 0))
    row = pl.BlockSpec((1, tile), lambda i: (0, i))
    return pl.pallas_call(
        functools.partial(joint_kernel, min(512, length)),
        grid=(width // tile,),
        in_specs=[
            whole(dqkv),
            whole(dpre),
            pl.BlockSpec((tile, cols), lambda i: (i, 0)),
            pl.BlockSpec((length, tile), lambda i: (0, i)),
            whole(mean),
            whole(inv),
            row,
            row,
        ],
        out_specs=[pl.BlockSpec((length, tile), lambda i: (0, i)), pl.BlockSpec((4, tile), lambda i: (0, i))],
        out_shape=[
            jax.ShapeDtypeStruct((length, width), jnp.bfloat16),
            jax.ShapeDtypeStruct((4, width), jnp.float32),
        ],
        cost_estimate=pl.CostEstimate(
            flops=2 * length * width * cols,
            bytes_accessed=2 * (width * cols + length * cols + 2 * length * width),
            transcendentals=0,
        ),
        name="joint_sum",
    )(dqkv, dpre, w, x, mean, inv, gain1, gain2)


def grads_kernel(blocks, same, ids_ref, *refs):
    lefts, rights = refs[: 1 if same else 2], refs[1 if same else 2 : -2]
    mates_ref, mine_ref = refs[-2:]
    step = pl.program_id(0)

    def write(out_ref):
        at = 0
        for k, right in enumerate(rights):
            left = lefts[0 if same else k]
            out_ref[0, :, at : at + right.shape[1]] = contract_first(left[...], right[...]).astype(jnp.bfloat16)
            at += right.shape[1]

    @pl.when(step < blocks)
    def _():
        write(mates_ref)

    @pl.when(step >= blocks)
    def _():
        write(mine_ref)


def weight_grads(ids, lefts, rights, shard, name):
    length, width = lefts[0].shape
    steps = width // shard
    blocks = steps // CORES
    cols = sum(r.shape[1] for r in rights)
    grid_spec = pltpu.PrefetchScalarGridSpec(
        num_scalar_prefetch=1,
        grid=(steps,),
        in_specs=[pl.BlockSpec((length, shard), lambda i, ids: (0, ids[i]))] * len(lefts)
        + [pl.BlockSpec(r.shape, lambda i, ids: (0, 0)) for r in rights],
        out_specs=[
            pl.BlockSpec((1, shard, cols), lambda i, ids: (jnp.minimum(i, blocks - 1), 0, 0)),
            pl.BlockSpec((1, shard, cols), lambda i, ids: (jnp.maximum(i - blocks, 0), 0, 0)),
        ],
    )
    return pl.pallas_call(
        functools.partial(grads_kernel, blocks, len(lefts) == 1),
        grid_spec=grid_spec,
        out_shape=[jax.ShapeDtypeStruct((blocks, shard, cols), jnp.bfloat16)] * 2,
        cost_estimate=pl.CostEstimate(
            flops=2 * length * width * cols,
            bytes_accessed=2 * (width * cols + length * cols + length * width * len(lefts)),
            transcendentals=0,
        ),
        name=name,
    )(ids, *lefts, *rights)


def ring_scatter(block_of, shift, n):
    to_bf16 = lambda a: a.astype(jnp.bfloat16)
    wide = lambda a: a.astype(jnp.float32)
    far = block_of(n // 2)
    half = far.shape[0] // 2
    right, left = shift(to_bf16(far[:half]), 1), shift(to_bf16(far[half:]), -1)
    for k in range(n // 2 - 1, 0, -1):
        ahead, behind = block_of(k), block_of(-k)
        if right.shape[0] == half:
            ahead = jnp.concatenate([ahead[:half] + wide(right), ahead[half:]])
            behind = jnp.concatenate([behind[:half], behind[half:] + wide(left)])
        else:
            ahead, behind = ahead + wide(right), behind + wide(left)
        right, left = shift(to_bf16(ahead), 1), shift(to_bf16(behind), -1)
    return block_of(0) + wide(right) + wide(left)


def summed(vector, axis):
    n = lax.axis_size(axis)
    bit = 1
    while bit < n:
        vector = vector + lax.ppermute(vector, axis, [(i, i ^ bit) for i in range(n)])
        bit *= 2
    return vector


def gelu_value(pre_act):
    return 0.5 * pre_act * (1.0 + lax.erf(pre_act * erf_scale))


def gelu_slope(pre_act):
    return (
        0.5 * (1.0 + lax.erf(pre_act * erf_scale))
        + pre_act * jnp.exp(-0.5 * pre_act * pre_act) * normal_peak
    )


def per_device(
    inputs,
    segments,
    first_gain,
    first_shift,
    second_gain,
    second_shift,
    qkv_weight,
    qkv_bias,
    dense_weight,
    dense_bias,
    fc_weight,
    fc_bias,
    proj_weight,
    proj_bias,
    cotangent,
):
    shard, heads, _, hd = qkv_weight.shape
    width = inputs.shape[1]
    rows = inputs.shape[0]
    nz, nd = lax.axis_size("tensor"), lax.axis_size("dp")
    nr = nd // CORES
    length = segments.shape[1]
    z, dp = lax.axis_index("tensor"), lax.axis_index("dp")
    chip, core = dp // CORES, dp % CORES
    f32, bf16 = jnp.float32, jnp.bfloat16

    all_in = lax.all_gather(inputs, "tensor", axis=0, tiled=True)
    all_cot = lax.all_gather(cotangent, "tensor", axis=0, tiled=True)
    w_in, w_out = gather_weights(
        (qkv_weight.reshape(shard, heads * 3 * hd), fc_weight, dense_weight, proj_weight)
    )
    segment = segments[0]
    tables = rotary_tables(segment, 128)
    qkv_cols, ctx_cols = heads * 3 * hd, heads * hd
    block_rows = min(256, length)

    r_order = static_order("comb", nr)
    r_place = comb_place(chip, nr)
    places = comb_at((r_place + jnp.arange(nr, dtype=jnp.int32)) % nr, nr) * CORES
    ids = jnp.concatenate([places + 1 - core, places + core]).astype(jnp.int32)

    def r_shift(a, d):
        pairs = [
            (r_order[i] * CORES + c, r_order[(i + d) % nr] * CORES + c) for i in range(nr) for c in range(CORES)
        ]
        return lax.ppermute(a, "dp", pairs)

    def scatter_rows(a):
        return lax.psum_scatter(a, "tensor", scatter_dimension=0, tiled=True).astype(f32)

    def weight_scatter(mates, mine):
        got = lax.ppermute(mates, "dp", [(i, i ^ 1) for i in range(nd)])
        return ring_scatter(lambda k: mine[k % nr].astype(f32) + got[k % nr].astype(f32), r_shift, nr)

    vectors = [a[None] for a in (first_gain, first_shift, second_gain, second_shift)]
    bias = jnp.concatenate([qkv_bias.reshape(-1), fc_bias])[None]
    qkv_rows, activated, slope, first_normed, second_normed, mean, inv_scale = front(
        all_in, w_in, bias, vectors, qkv_cols
    )
    *saved, log_total = attend(qkv_rows, tables, segment, heads, hd, block_rows, length // 2)
    context = saved[3]
    mixed_part = mix(context, activated, w_out)
    mixed_part, all_cot = lax.optimization_barrier((mixed_part, all_cot))
    mixed = scatter_rows(mixed_part)
    output = (inputs.astype(f32) + mixed + dense_bias + proj_bias).astype(bf16)

    grads_out = weight_grads(ids, [all_cot], [context, activated], shard, "grads_out")
    grad_out = weight_scatter(*grads_out)
    dense_weight_grad, proj_weight_grad = grad_out[:, :ctx_cols], grad_out[:, ctx_cols:]
    d_context, d_pre_half, fc_bias_part = back(all_cot, w_out, slope, ctx_cols)
    d_qkv_half, qkv_bias_part = attend_back(
        saved, log_total, d_context, tables, segment, heads, hd, block_rows, length // 2
    )
    joint, gains = joint_sum(d_qkv_half, d_pre_half, w_in, all_in, mean, inv_scale, vectors[0], vectors[2])
    joint, d_qkv_late, d_pre_late = lax.optimization_barrier((joint, d_qkv_half, d_pre_half))
    joint_rows = scatter_rows(joint)
    grads_in = weight_grads(ids, [first_normed, second_normed], [d_qkv_late, d_pre_late], shard, "grads_in")
    grad_in = weight_scatter(*grads_in)
    qkv_weight_grad, fc_weight_grad = grad_in[:, :qkv_cols], grad_in[:, qkv_cols:]

    own = lambda a: lax.dynamic_slice_in_dim(a, z * rows, rows, axis=0)
    own_unit = (inputs.astype(f32) - own(mean)) * own(inv_scale)
    first_mean = jnp.mean(joint_rows, axis=-1, keepdims=True)
    second_mean = jnp.mean(joint_rows * own_unit, axis=-1, keepdims=True)
    input_grad = (
        cotangent.astype(f32) + own(inv_scale) * (joint_rows - first_mean - own_unit * second_mean)
    ).astype(bf16)

    gains = summed(summed(gains, "dp"), "tensor")
    early = jnp.concatenate([jnp.sum(all_cot.astype(f32), axis=0), fc_bias_part[0], qkv_bias_part[0]])
    early = summed(early, "dp")
    bias_total = early[:width]
    fc_bias_grad = early[width : width + fc_bias.shape[0]]
    qkv_bias_grad = early[width + fc_bias.shape[0] :].reshape(qkv_bias.shape)
    return (
        output,
        input_grad,
        gains[0],
        gains[1],
        gains[2],
        gains[3],
        qkv_weight_grad.reshape(qkv_weight.shape),
        qkv_bias_grad,
        dense_weight_grad,
        bias_total,
        fc_weight_grad,
        fc_bias_grad,
        proj_weight_grad,
        bias_total,
    )


def solution(mesh):
    both = P(("dp", "tensor"), None)
    return jax.shard_map(
        per_device,
        mesh=mesh,
        in_specs=(
            both,
            P("dp", None),
            P(),
            P(),
            P(),
            P(),
            P("dp", "tensor", None, None),
            P("tensor", None, None),
            P("dp", "tensor"),
            P(),
            P("dp", "tensor"),
            P("tensor"),
            P("dp", "tensor"),
            P(),
            both,
        ),
        out_specs=(
            both,
            both,
            P(),
            P(),
            P(),
            P(),
            P("dp", "tensor", None, None),
            P("tensor", None, None),
            P("dp", "tensor"),
            P(),
            P("dp", "tensor"),
            P("tensor"),
            P("dp", "tensor"),
            P(),
        ),
        check_vma=False,
    )
```
